32 devices in a mesh: section: 2 (over y), dp: 16 (over z, x, core).
Axes of the slice: x: 2, y: 2, z: 4, core: 2. Of those that a mesh axis runs over, the one named last changes fastest.
Arguments:
- student_head_logits: bfloat16 [32, 64, 32768], P('dp', None, 'section'), may hold values from -40 to 300
- hidden: bfloat16 [32, 64, 4096], P('dp', None, 'section'), may hold values from -6 to 6
- adapter_down: bfloat16 [4096, 32], P('section'), may hold values from -0.09375 to 0.09375
- adapter_up: bfloat16 [32, 32768], P(None, 'section'), may hold values from -1 to 1
- teacher_top_index: int32 [32, 64, 32], P('dp'), may hold values from 0 to 32767, as said below
- teacher_top_values: float32 [32, 64, 32], P('dp'), may hold values from -40 to 300
- teacher_other_logit: float32 [32, 64], P('dp'), may hold values from -40 to 300
- lengths: int32 [32], P('dp'), may hold values from 1 to 64, as said below
Outputs:
- distill_loss: float32 [], replicated
- grad_lora_a: float32 [4096, 32], P('section')
- grad_lora_b: float32 [32, 32768], P(None, 'section')
The draws below stay inside these ranges and needn't reach their ends.
Inputs may be any that keep to these rules, and one draw needn't show every extreme that they name: `teacher_top_index`: the 32 ids of one position are distinct. `lengths`: the last sequence has all 64 positions sampled.
All inputs are finite; a program needn't handle non-finite values.
Results may differ from the reference program's by a relative error of at most 0.019.
Values may be sent and summed in bfloat16 or wider, within the bound.
A program may use at most 128 MiB of HBM per device.

```python
import jax
import jax.numpy as jnp
from jax import lax

MODEL_WIDTH = 4096
VOCAB_SIZE = 32768
ADAPTER_RANK = 32
TOPK = 32
LEN = 64
SEQ_DEV = 2
SEQS = 32
N_SECTION = 2


def index_table(key):
    start_key, stride_key = jax.random.split(jax.random.fold_in(key, 11))
    start_ids = jax.random.randint(start_key, (SEQS, LEN, 1), 0, VOCAB_SIZE)
    index_steps = jax.random.randint(stride_key, (SEQS, LEN, TOPK), 1, VOCAB_SIZE // TOPK)
    return (start_ids + jnp.cumsum(index_steps, axis=2)) % VOCAB_SIZE


def draw_teacher_top_index(key, part):
    return index_table(key).astype(jnp.int32)


def draw_student_head_logits(key, part):
    noise_key, boost_key = jax.random.split(jax.random.fold_in(key, 12), 2)
    noise_part = 3.0 * jax.random.normal(noise_key, (SEQS, LEN, VOCAB_SIZE))
    token_ids = index_table(key)
    support_boost = jax.random.uniform(boost_key, (SEQS, LEN, TOPK), minval=9.0, maxval=14.0)
    seq_ids = jnp.arange(SEQS)[:, None, None]
    pos_ids = jnp.arange(LEN)[None, :, None]
    output_logits = noise_part.at[seq_ids, pos_ids, token_ids].add(support_boost)
    return output_logits.astype(jnp.bfloat16)


def teacher_pair(key):
    value_key, rest_key = jax.random.split(jax.random.fold_in(key, 13), 2)
    values = 4.0 + 2.0 * jax.random.normal(value_key, (SEQS, LEN, TOPK))
    rest_logit = 2.0 + 1.5 * jax.random.normal(rest_key, (SEQS, LEN))
    return (values, rest_logit)


def draw_teacher_top_values(key, part):
    return teacher_pair(key)[0].astype(jnp.float32)


def draw_teacher_other_logit(key, part):
    return teacher_pair(key)[1].astype(jnp.float32)


def draw_lengths(key, part):
    shard_ids = jnp.arange(SEQS, dtype=jnp.int32) // SEQ_DEV
    shard_total = SEQS // SEQ_DEV
    length_cap = LEN // 3 + (LEN - LEN // 3) * shard_ids // max(shard_total - 1, 1)
    lower_end = jnp.maximum(length_cap // 2, 1)
    length_draw = jax.random.randint(jax.random.fold_in(key, 14), (SEQS,), lower_end, length_cap + 1)
    return length_draw.at[SEQS - 1].set(LEN).astype(jnp.int32)


def block_levels(key, extent, cuts, least, top_value):
    loudness = 1.0
    for dim, shards_of in cuts:
        heights = jax.random.uniform(jax.random.fold_in(jax.random.fold_in(key, 6), dim), (shards_of,), jnp.float32, least / len(cuts), top_value / len(cuts))
        loudness = loudness * jnp.repeat(jnp.exp(heights), extent[dim] // shards_of).reshape((-1,) + (1,) * (len(extent) - 1 - dim))
    return loudness


def scatter_about(rng, dims, spread, most, shards=(), kind=jnp.bfloat16):
    loudness = block_levels(rng, dims, shards, -0.22, 0.18) if shards else 1.0
    entries = jax.random.normal(rng, dims, jnp.float32) * spread * loudness
    return jnp.minimum(jnp.maximum(entries, -most), most).astype(kind)


def setup_inputs(seed: int = 0) -> dict:
    splits = jax.random.split(jax.random.key(seed), 9)
    return {
        "student_head_logits": draw_student_head_logits(jax.random.fold_in(splits[8], 71), 0),
        "hidden": scatter_about(splits[1], (SEQS, LEN, MODEL_WIDTH), 1.0, 6.0, ((0, 16), (2, 2))),
        "adapter_down": scatter_about(splits[2], (MODEL_WIDTH, ADAPTER_RANK), MODEL_WIDTH ** -0.5, 0.09375, ((0, 2),)),
        "adapter_up": scatter_about(splits[3], (ADAPTER_RANK, VOCAB_SIZE), ADAPTER_RANK ** -0.5, 1.0, ((1, 2),)),
        "teacher_top_index": draw_teacher_top_index(jax.random.fold_in(splits[8], 71), 0),
        "teacher_top_values": draw_teacher_top_values(jax.random.fold_in(splits[8], 71), 0),
        "teacher_other_logit": draw_teacher_other_logit(jax.random.fold_in(splits[8], 71), 0),
        "lengths": draw_lengths(jax.random.fold_in(splits[8], 71), 0),
    }


SCALE_LOSS = 16384.0


def contract_rows(former, latter):
    return lax.dot_general(former.astype(jnp.float32), latter.astype(jnp.float32), (((0,), (0,)), ((), ())), precision=lax.Precision.HIGHEST)


def section_sum(partials):
    rounded = lax.optimization_barrier(partials.astype(jnp.bfloat16))
    return jnp.sum(rounded.astype(jnp.float32), axis=0).astype(jnp.bfloat16)


def reference(student_head_logits, hidden, adapter_down, adapter_up, teacher_top_index, teacher_top_values, teacher_other_logit, lengths):
    row_ids = jnp.arange(LEN, dtype=jnp.int32)[:, None]
    position = jnp.arange(LEN, dtype=jnp.int32)
    down_blocks = adapter_down.astype(jnp.float32).reshape(N_SECTION, MODEL_WIDTH // N_SECTION, ADAPTER_RANK)
    up_blocks = adapter_up.astype(jnp.float32).reshape(ADAPTER_RANK, N_SECTION, VOCAB_SIZE // N_SECTION)

    def per_sequence(scan_carry, scan_item):
        grad_a, grad_b, loss_sum = scan_carry
        output_logits, hidden_features, token_ids, values, rest_logit, length = scan_item
        feature_blocks = hidden_features.astype(jnp.float32).reshape(LEN, N_SECTION, MODEL_WIDTH // N_SECTION)
        low_partials = jnp.einsum("lsw,swr->slr", feature_blocks, down_blocks, precision=lax.Precision.HIGHEST)
        reduced_features = section_sum(low_partials)
        logit_scores = output_logits.astype(jnp.float32) + jnp.dot(reduced_features, adapter_up, preferred_element_type=jnp.float32)
        row_top = jnp.max(logit_scores, axis=1)
        exp_scores = jnp.exp(logit_scores - row_top[:, None])
        support = jnp.zeros((LEN, VOCAB_SIZE), jnp.float32).at[row_ids, token_ids].set(1.0)
        row_total = jnp.sum(exp_scores, axis=1)
        tail_mass = jnp.sum(exp_scores * (1.0 - support), axis=1)
        picked = jnp.take_along_axis(logit_scores, token_ids, axis=1)
        log_total = jnp.log(row_total)
        log_q = picked - row_top[:, None] - log_total[:, None]
        log_q_tail = jnp.log(tail_mass) - log_total
        teacher_top = jnp.maximum(jnp.max(values, axis=1), rest_logit)
        teacher_norm = jnp.log(jnp.sum(jnp.exp(values - teacher_top[:, None]), axis=1) + jnp.exp(rest_logit - teacher_top)) + teacher_top
        log_ratio = log_q - (values - teacher_norm[:, None])
        log_ratio_tail = log_q_tail - (rest_logit - teacher_norm)
        divergence = jnp.sum(jnp.exp(log_q) * log_ratio, axis=1) + jnp.exp(log_q_tail) * log_ratio_tail
        valid_mask = (position < length).astype(jnp.float32)
        student_prob = exp_scores / row_total[:, None]
        log_gap = jnp.broadcast_to(log_ratio_tail[:, None], (LEN, VOCAB_SIZE)).at[row_ids, token_ids].set(log_ratio)
        score_gradient = (valid_mask[:, None] * student_prob * (log_gap - divergence[:, None])).astype(jnp.bfloat16)
        gradient_blocks = score_gradient.astype(jnp.float32).reshape(LEN, N_SECTION, VOCAB_SIZE // N_SECTION)
        back_partials = jnp.einsum("lsv,rsv->slr", gradient_blocks, up_blocks, precision=lax.Precision.HIGHEST)
        reduced_gradient = section_sum(back_partials)
        grad_a = grad_a + contract_rows(hidden_features, reduced_gradient)
        grad_b = grad_b + contract_rows(reduced_features, score_gradient)
        loss_sum = loss_sum + jnp.sum(valid_mask * divergence)
        return (grad_a, grad_b, loss_sum), None

    start_state = (jnp.zeros((MODEL_WIDTH, ADAPTER_RANK), jnp.float32), jnp.zeros((ADAPTER_RANK, VOCAB_SIZE), jnp.float32), jnp.zeros((), jnp.float32))
    final_state, _ = lax.scan(per_sequence, start_state, (student_head_logits, hidden, teacher_top_index, teacher_top_values, teacher_other_logit, lengths))
    grad_a, grad_b, loss_sum = final_state
    token_count = jnp.sum(lengths).astype(jnp.float32)
    return loss_sum / token_count, grad_a * SCALE_LOSS / token_count, grad_b * SCALE_LOSS / token_count
```

```python
import functools

import jax
import jax.numpy as jnp
from jax import lax
from jax.experimental import pallas as pl
from jax.experimental.pallas import tpu as pltpu
from jax.sharding import PartitionSpec as P

SCALE_LOSS = 16384.0
LANES = 128
F32 = jnp.float32
BF16 = jnp.bfloat16
MESH = pl.DeviceIdType.MESH


def remote(src, dst, send, recv, axis, target):
    return pltpu.make_async_remote_copy(
        src_ref=src,
        dst_ref=dst,
        send_sem=send,
        recv_sem=recv,
        device_id={axis: target},
        device_id_type=MESH,
    )


class SectionExchange:
    def __init__(self, buf, send, recv, n):
        self.buf = buf
        me = lax.axis_index("section")
        self.copies = [
            remote(buf.at[me], buf.at[me], send.at[j - 1], recv.at[j - 1], "section", lax.rem(me + j, n))
            for j in range(1, n)
        ]

    def start(self):
        for c in self.copies:
            c.start()

    def wait(self):
        for c in self.copies:
            c.wait()


class DataReduce:
    def __init__(self, part, pair, slots, total, sems, n):
        self.part, self.pair, self.slots, self.total = part, pair, slots, total
        self.sems = sems
        self.n2 = n // 2
        self.width = part.shape[1] // n
        self.half = part.shape[1] // 2
        me = lax.axis_index("dp")
        self.core = lax.rem(me, 2)
        self.chip = me // 2
        self.mate = me + 1 - 2 * self.core

    def peer(self, j):
        return lax.rem(self.chip + j, self.n2) * 2 + self.core

    def cols(self, half, piece):
        start = pl.multiple_of(half * self.half + piece * self.width, LANES)
        return pl.ds(start, self.width)

    def order(self):
        return list(range(1, self.n2)) + [0]

    def start_pair(self):
        self.pair_copies = {}
        for j in self.order():
            piece = lax.rem(self.chip + j, self.n2)
            c = remote(
                self.part.at[:, self.cols(1 - self.core, piece)],
                self.pair.at[:, self.cols(0, piece)],
                self.sems.at[0, j],
                self.sems.at[1, j],
                "dp",
                self.mate,
            )
            c.start()
            self.pair_copies[j] = c

    def start_scatter(self):
        self.scatter_copies = {}
        for j in self.order():
            piece = lax.rem(self.chip + j, self.n2)
            self.pair_copies[j].wait()
            mine = self.cols(self.core, piece)
            both = self.part[:, mine].astype(F32) + self.pair[:, self.cols(0, piece)].astype(F32)
            self.part[:, mine] = both.astype(BF16)
            if j:
                c = remote(
                    self.part.at[:, mine],
                    self.slots.at[j - 1],
                    self.sems.at[2, j],
                    self.sems.at[3, j],
                    "dp",
                    self.peer(j),
                )
                c.start()
                self.scatter_copies[j] = c

    def start_gather(self):
        mine = self.cols(self.core, self.chip)
        acc = self.part[:, mine].astype(F32)
        for j in range(1, self.n2):
            self.scatter_copies[j].wait()
            acc = acc + self.slots[j - 1].astype(F32)
        self.total[:, mine] = acc.astype(BF16)
        self.gather_copies = {}
        for j in self.order():
            c = remote(
                self.total.at[:, mine],
                self.total.at[:, mine],
                self.sems.at[4, j],
                self.sems.at[5, j],
                "dp",
                self.peer(j) if j else self.mate,
            )
            c.start()
            self.gather_copies[j] = c

    def forward(self):
        forwards = []
        for j in range(1, self.n2):
            piece = lax.rem(self.chip + self.n2 - j, self.n2)
            theirs = self.cols(self.core, piece)
            self.gather_copies[j].wait()
            c = remote(
                self.total.at[:, theirs],
                self.total.at[:, theirs],
                self.sems.at[6, j],
                self.sems.at[7, j],
                "dp",
                self.mate,
            )
            c.start()
            forwards.append(c)
        self.gather_copies[0].wait()
        for c in forwards:
            c.wait()


def contract(former, latter, dims):
    return lax.dot_general(former, latter, (dims, ((), ())), preferred_element_type=F32)


def kernel(
    n_sec,
    n_dp,
    seq_len,
    lengths_ref,
    logits_ref,
    hidden_ref,
    down_ref,
    up_ref,
    ids_ref,
    values_ref,
    other_ref,
    loss_ref,
    grad_a_ref,
    grad_b_ref,
    scores_ref,
    teach_ref,
    grad_ref,
    hi_ref,
    lo_ref,
    piece_ref,
    low_buf,
    stat_buf,
    back_buf,
    acc_ref,
    row_ref,
    b_part,
    b_pair,
    b_slots,
    b_total,
    a_part,
    a_pair,
    a_slots,
    a_total,
    loss_part,
    loss_slots,
    sec_send,
    sec_recv,
    b_sems,
    a_sems,
    loss_sems,
):
    rows, width = logits_ref.shape
    features = hidden_ref.shape[1]
    topk = ids_ref.shape[1]
    rank = up_ref.shape[0]
    blocks = width // LANES
    sec = lax.axis_index("section")
    me = lax.axis_index("dp")
    n2 = n_dp // 2
    core = lax.rem(me, 2)
    chip = me // 2
    mate = me + 1 - 2 * core

    barrier = pltpu.get_barrier_semaphore()
    for j in range(1, n_sec):
        pl.semaphore_signal(barrier, inc=1, device_id={"section": lax.rem(sec + j, n_sec)}, device_id_type=MESH)
    pl.semaphore_signal(barrier, inc=1, device_id={"dp": mate}, device_id_type=MESH)
    for j in range(1, n2):
        pl.semaphore_signal(
            barrier, inc=1, device_id={"dp": lax.rem(chip + j, n2) * 2 + core}, device_id_type=MESH
        )

    low_part = jnp.dot(hidden_ref[...], down_ref[...], preferred_element_type=F32)
    low_buf[sec] = low_part.astype(BF16)
    pl.semaphore_wait(barrier, n_sec - 1 + 1 + n2 - 1)
    low_swap = SectionExchange(low_buf, sec_send.at[0], sec_recv.at[0], n_sec)
    low_swap.start()

    values = values_ref[...]
    seq_total = rows // seq_len
    eye = lax.broadcasted_iota(jnp.int32, (seq_len, seq_len), 0) == lax.broadcasted_iota(
        jnp.int32, (seq_len, seq_len), 1
    )
    rest = jnp.concatenate(
        [
            jnp.sum(jnp.where(eye, jnp.broadcast_to(other_ref[s : s + 1, :], (seq_len, seq_len)), 0.0), axis=1, keepdims=True)
            for s in range(seq_total)
        ],
        axis=0,
    )
    teacher_top = jnp.maximum(jnp.max(values, axis=1, keepdims=True), rest)
    teacher_norm = (
        jnp.log(jnp.sum(jnp.exp(values - teacher_top), axis=1, keepdims=True) + jnp.exp(rest - teacher_top))
        + teacher_top
    )
    log_t_tail = rest - teacher_norm
    shifted = jnp.minimum(values - teacher_norm, 0.0) - 1.0
    first = shifted.astype(BF16).astype(F32)
    second = (shifted - first).astype(BF16).astype(F32)
    third = shifted - first - second
    ids = ids_ref[...]
    high = ((ids >> 7) - sec * blocks).astype(F32)
    low = (ids & (LANES - 1)).astype(F32)
    hi_ref[...] = jnp.full((rows, LANES), -1.0, F32)
    lo_ref[...] = jnp.full((rows, LANES), -1.0, F32)
    piece_ref[...] = jnp.zeros((rows, LANES), F32)
    for i, piece in enumerate((first, second, third)):
        span = slice(i * topk, (i + 1) * topk)
        hi_ref[:, span] = high
        lo_ref[:, span] = low
        piece_ref[:, span] = piece
    block_iota = lax.broadcasted_iota(jnp.int32, (blocks, LANES), 0).astype(F32)
    lane_iota = lax.broadcasted_iota(jnp.int32, (LANES, LANES), 0).astype(F32)

    def place_row(r):
        left = jnp.where(block_iota == hi_ref[pl.ds(r, 1), :], piece_ref[pl.ds(r, 1), :], 0.0)
        right = jnp.where(lane_iota == lo_ref[pl.ds(r, 1), :], 1.0, 0.0)
        teach_ref[pl.ds(r, blocks, stride=rows), :] = contract(
            left.astype(BF16), right.astype(BF16), ((1,), (1,))
        )

    unroll = 4

    @pl.loop(0, rows // unroll)
    def _(step):
        for u in range(unroll):
            place_row(step * unroll + u)

    low_swap.wait()
    low_sum = low_buf[0].astype(F32)
    for s in range(1, n_sec):
        low_sum = low_sum + low_buf[s].astype(F32)
    low_rank = low_sum.astype(BF16)
    low_rank_t = low_sum.T.astype(BF16)

    span = 256

    def score_step(step, top):
        cols = pl.ds(pl.multiple_of(step * span, span), span)
        block = logits_ref[:, cols].astype(F32) + jnp.dot(
            low_rank, up_ref[:, cols], preferred_element_type=F32
        )
        scores_ref[:, cols] = block
        for i in range(span // LANES):
            top = jnp.maximum(top, block[:, i * LANES : (i + 1) * LANES])
        return top

    top = lax.fori_loop(
        0, width // span, score_step, jnp.full((rows, LANES), -3.0e38, F32), unroll=2
    )
    local_top = jnp.max(top, axis=1, keepdims=True)
    row_ref[0] = jnp.broadcast_to(local_top, (rows, LANES))

    group = 32
    lane = lax.broadcasted_iota(jnp.int32, (group, LANES), 1)
    chunk = 4

    @pl.loop(0, rows // group)
    def _(g):
        base = pl.multiple_of(g * group, group)
        here = pl.ds(base, group)
        peak = row_ref[0, here, :]

        def step_sum(step, carry):
            total, tail, mass, cross = carry
            for i in range(chunk):
                b = step * chunk + i
                s = scores_ref[here, pl.ds(pl.multiple_of(b * LANES, LANES), LANES)]
                t = teach_ref[pl.ds(pl.multiple_of(b * rows + base, group), group), :]
                gap = s - peak
                e = jnp.exp(gap)
                named = t < 0.0
                e_named = jnp.where(named, e, 0.0)
                total = total + e
                tail = tail + jnp.where(named, 0.0, e)
                mass = mass + e_named
                cross = cross + e_named * (gap - t)
            return total, tail, mass, cross

        zero = jnp.zeros((group, LANES), F32)
        sums = lax.fori_loop(0, blocks // chunk, step_sum, (zero, zero, zero, zero))
        packed = peak
        for i, x in enumerate(sums):
            packed = jnp.where(lane == i + 1, jnp.sum(x, axis=1, keepdims=True), packed)
        stat_buf[sec, here, :] = packed

    stat_swap = SectionExchange(stat_buf, sec_send.at[1], sec_recv.at[1], n_sec)
    stat_swap.start()
    position = lax.broadcasted_iota(jnp.int32, (seq_len, 1), 0)
    valid = jnp.concatenate(
        [(position < lengths_ref[s]).astype(F32) for s in range(seq_total)], axis=0
    )
    count = lengths_ref[0]
    for s in range(1, seq_total):
        count = count + lengths_ref[s]
    stat_swap.wait()

    tops = [stat_buf[s, :, 0:1] for s in range(n_sec)]
    row_top = functools.reduce(jnp.maximum, tops)
    shrink = [jnp.exp(t - row_top) for t in tops]
    row_total = sum(stat_buf[s, :, 1:2] * shrink[s] for s in range(n_sec))
    tail_mass = sum(stat_buf[s, :, 2:3] * shrink[s] for s in range(n_sec))
    log_total = jnp.log(row_total)
    log_tail = jnp.log(tail_mass) - log_total
    tail_ratio = log_tail - log_t_tail
    divergence = jnp.exp(log_tail) * tail_ratio
    for s in range(n_sec):
        shift = tops[s] - row_top - log_total - 1.0
        divergence = divergence + (shrink[s] / row_total) * (
            stat_buf[s, :, 4:5] + stat_buf[s, :, 3:4] * shift
        )
    own_shift = local_top - row_top - log_total - 1.0
    full = (rows, LANES)
    row_ref[1] = jnp.broadcast_to(valid * jnp.exp(local_top - row_top) / row_total, full)
    row_ref[2] = jnp.broadcast_to(own_shift - divergence, full)
    row_ref[3] = jnp.broadcast_to(tail_ratio - divergence, full)

    loss_sum = jnp.sum(valid * divergence, axis=0, keepdims=True)
    tile_lane = lax.broadcasted_iota(jnp.int32, (8, LANES), 1)
    loss_part[0] = jnp.where(tile_lane == 0, loss_sum, jnp.where(tile_lane == 1, count.astype(F32), 0.0))
    loss_pair = remote(loss_part.at[0], loss_part.at[1], loss_sems.at[0, 0], loss_sems.at[1, 0], "dp", mate)
    loss_pair.start()

    acc_ref[...] = jnp.zeros_like(acc_ref)
    if b_part.shape[1] > width:
        b_part[:, width:] = jnp.zeros((rank, b_part.shape[1] - width), BF16)
    if a_part.shape[1] > features:
        a_part[:, features:] = jnp.zeros((rank, a_part.shape[1] - features), BF16)
    wide = 512

    @pl.loop(0, width // wide)
    def _(step):
        for g in range(rows // group):
            here = pl.ds(g * group, group)
            peak, scale = row_ref[0, here, :], row_ref[1, here, :]
            named_add, tail_add = row_ref[2, here, :], row_ref[3, here, :]
            for i in range(wide // LANES):
                b = step * (wide // LANES) + i
                s = scores_ref[here, pl.ds(pl.multiple_of(b * LANES, LANES), LANES)]
                t = teach_ref[pl.ds(pl.multiple_of(b * rows + g * group, group), group), :]
                gap = s - peak
                coef = jnp.where(t < 0.0, gap - t + named_add, tail_add)
                grad_ref[here, i * LANES : (i + 1) * LANES] = (jnp.exp(gap) * scale * coef).astype(BF16)
        cols = pl.ds(pl.multiple_of(step * wide, wide), wide)
        g_block = grad_ref[...]
        acc_ref[...] += contract(g_block, up_ref[:, cols], ((1,), (1,)))
        b_part[:, cols] = jnp.dot(low_rank_t, g_block, preferred_element_type=F32).astype(BF16)

    back_buf[sec] = acc_ref[...].astype(BF16)
    back_swap = SectionExchange(back_buf, sec_send.at[2], sec_recv.at[2], n_sec)
    back_swap.start()
    b_sum = DataReduce(b_part, b_pair, b_slots, b_total, b_sems, n_dp)
    a_sum = DataReduce(a_part, a_pair, a_slots, a_total, a_sems, n_dp)
    b_sum.start_pair()

    loss_pair.wait()
    loss_part[2] = loss_part[0] + loss_part[1]
    loss_copies = []
    for j in range(1, n2):
        c = remote(
            loss_part.at[2],
            loss_slots.at[j - 1],
            loss_sems.at[0, j],
            loss_sems.at[1, j],
            "dp",
            lax.rem(chip + j, n2) * 2 + core,
        )
        c.start()
        loss_copies.append(c)

    b_sum.start_scatter()
    back_swap.wait()
    back_sum = back_buf[0].astype(F32)
    for s in range(1, n_sec):
        back_sum = back_sum + back_buf[s].astype(F32)
    back_t = back_sum.T.astype(BF16)
    a_part[:, 0:features] = jnp.dot(back_t, hidden_ref[...], preferred_element_type=F32).astype(BF16)
    a_sum.start_pair()
    a_sum.start_scatter()
    b_sum.start_gather()
    a_sum.start_gather()

    loss_all = loss_part[2]
    for j in range(1, n2):
        loss_copies[j - 1].wait()
        loss_all = loss_all + loss_slots[j - 1]
    count_all = loss_all[0:1, 1:2]
    loss_ref[...] = loss_all / count_all
    factor = SCALE_LOSS / count_all

    b_sum.forward()
    a_sum.forward()
    grad_b_ref[...] = b_total[:, 0:width].astype(F32) * factor
    grad_a_ref[...] = a_total[:, 0:features].astype(F32) * factor


def padded(columns, n):
    unit = LANES * n
    return (columns + unit - 1) // unit * unit


def body(
    n_sec,
    n_dp,
    student_head_logits,
    hidden,
    adapter_down,
    adapter_up,
    teacher_top_index,
    teacher_top_values,
    teacher_other_logit,
    lengths,
):
    seq_total, seq_len, width = student_head_logits.shape
    rows = seq_total * seq_len
    features = hidden.shape[2]
    topk = teacher_top_index.shape[2]
    rank = adapter_up.shape[0]
    n2 = n_dp // 2
    b_width, a_width = padded(width, n_dp), padded(features, n_dp)
    vmem = pl.BlockSpec(memory_space=pltpu.VMEM)

    def reduce_scratch(columns):
        return [
            pltpu.VMEM((rank, columns), BF16),
            pltpu.VMEM((rank, columns // 2), BF16),
            pltpu.VMEM((n2 - 1, rank, columns // n_dp), BF16),
            pltpu.VMEM((rank, columns), BF16),
        ]

    loss, grad_a, grad_b = pl.pallas_call(
        functools.partial(kernel, n_sec, n_dp, seq_len),
        out_shape=(
            jax.ShapeDtypeStruct((8, LANES), F32),
            jax.ShapeDtypeStruct((rank, features), F32),
            jax.ShapeDtypeStruct((rank, width), F32),
        ),
        in_specs=[pl.BlockSpec(memory_space=pltpu.SMEM)] + [vmem] * 7,
        out_specs=(vmem, vmem, vmem),
        scratch_shapes=[
            pltpu.VMEM((rows, width), F32),
            pltpu.VMEM((rows * (width // LANES), LANES), F32),
            pltpu.VMEM((rows, 512), BF16),
            pltpu.VMEM((rows, LANES), F32),
            pltpu.VMEM((rows, LANES), F32),
            pltpu.VMEM((rows, LANES), F32),
            pltpu.VMEM((n_sec, rows, rank), BF16),
            pltpu.VMEM((n_sec, rows, LANES), F32),
            pltpu.VMEM((n_sec, rows, rank), BF16),
            pltpu.VMEM((rows, rank), F32),
            pltpu.VMEM((4, rows, LANES), F32),
            *reduce_scratch(b_width),
            *reduce_scratch(a_width),
            pltpu.VMEM((3, 8, LANES), F32),
            pltpu.VMEM((n2 - 1, 8, LANES), F32),
            pltpu.SemaphoreType.DMA((3, n_sec - 1)),
            pltpu.SemaphoreType.DMA((3, n_sec - 1)),
            pltpu.SemaphoreType.DMA((8, n2)),
            pltpu.SemaphoreType.DMA((8, n2)),
            pltpu.SemaphoreType.DMA((2, n2)),
        ],
        compiler_params=pltpu.CompilerParams(
            collective_id=0, has_side_effects=True, vmem_limit_bytes=60 * 1024 * 1024
        ),
    )(
        lengths,
        student_head_logits.reshape(rows, width),
        hidden.reshape(rows, features),
        adapter_down,
        adapter_up,
        teacher_top_index.reshape(rows, topk),
        teacher_top_values.reshape(rows, topk),
        teacher_other_logit,
    )
    return (loss[0, 0], grad_a.T, grad_b)


def solution(mesh):
    return jax.shard_map(
        functools.partial(body, mesh.shape["section"], mesh.shape["dp"]),
        mesh=mesh,
        in_specs=(
            P("dp", None, "section"),
            P("dp", None, "section"),
            P("section", None),
            P(None, "section"),
            P("dp", None, None),
            P("dp", None, None),
            P("dp", None),
            P("dp"),
        ),
        out_specs=(P(), P("section", None), P(None, "section")),
        check_vma=False,
    )
```

```python
import functools

import jax
import jax.numpy as jnp
from jax import lax
from jax.experimental import pallas as pl
from jax.experimental.pallas import tpu as pltpu
from jax.sharding import PartitionSpec as P

SCALE_LOSS = 16384.0
LANES = 128
SPAN = 1024
UNROLL = 16
SCALE_STEPS = 2
F32 = jnp.float32
BF16 = jnp.bfloat16
MESH = pl.DeviceIdType.MESH


def remote(src, dst, send, recv, axis, target):
    return pltpu.make_async_remote_copy(
        src_ref=src,
        dst_ref=dst,
        send_sem=send,
        recv_sem=recv,
        device_id={axis: target},
        device_id_type=MESH,
    )


class SectionExchange:
    def __init__(self, buf, send, recv, n):
        self.buf = buf
        me = lax.axis_index("section")
        self.copies = [
            remote(buf.at[me], buf.at[me], send.at[j - 1], recv.at[j - 1], "section", lax.rem(me + j, n))
            for j in range(1, n)
        ]

    def start(self):
        for c in self.copies:
            c.start()

    def wait(self):
        for c in self.copies:
            c.wait()


class DataReduce:
    def __init__(self, part, pair, slots, total, sems, n):
        self.part, self.pair, self.slots, self.total = part, pair, slots, total
        self.sems = sems
        self.n2 = n // 2
        self.width = part.shape[1] // n
        self.half = part.shape[1] // 2
        me = lax.axis_index("dp")
        self.core = lax.rem(me, 2)
        self.chip = me // 2
        self.mate = me + 1 - 2 * self.core

    def peer(self, j):
        return lax.rem(self.chip + j, self.n2) * 2 + self.core

    def cols(self, half, piece):
        start = pl.multiple_of(half * self.half + piece * self.width, LANES)
        return pl.ds(start, self.width)

    def order(self):
        return list(range(1, self.n2)) + [0]

    def pair_copy(self, j):
        piece = lax.rem(self.chip + j, self.n2)
        return remote(
            self.part.at[:, self.cols(1 - self.core, piece)],
            self.pair.at[:, self.cols(0, piece)],
            self.sems.at[0, j],
            self.sems.at[1, j],
            "dp",
            self.mate,
        )

    def start_pair(self):
        for j in self.order():
            self.pair_copy(j).start()

    def merge_piece(self, j):
        piece = lax.rem(self.chip + j, self.n2)
        self.pair_copy(j).wait()
        mine = self.cols(self.core, piece)
        both = self.part[:, mine].astype(F32) + self.pair[:, self.cols(0, piece)].astype(F32)
        self.part[:, mine] = both.astype(BF16)

    def scatter_copy(self, j):
        piece = lax.rem(self.chip + j, self.n2)
        return remote(
            self.part.at[:, self.cols(self.core, piece)],
            self.slots.at[j - 1],
            self.sems.at[2, j],
            self.sems.at[3, j],
            "dp",
            self.peer(j),
        )

    def start_scatter(self):
        for j in self.order():
            self.merge_piece(j)
            if j:
                self.scatter_copy(j).start()

    def start_gather(self):
        mine = self.cols(self.core, self.chip)
        acc = self.part[:, mine].astype(F32)
        for j in range(1, self.n2):
            self.scatter_copy(j).wait()
            acc = acc + self.slots[j - 1].astype(F32)
        self.total[:, mine] = acc.astype(BF16)
        self.gather_copies = {}
        for j in self.order():
            c = remote(
                self.total.at[:, mine],
                self.total.at[:, mine],
                self.sems.at[4, j],
                self.sems.at[5, j],
                "dp",
                self.peer(j) if j else self.mate,
            )
            c.start()
            self.gather_copies[j] = c

    def forward(self):
        forwards = []
        for j in range(1, self.n2):
            piece = lax.rem(self.chip + self.n2 - j, self.n2)
            theirs = self.cols(self.core, piece)
            self.gather_copies[j].wait()
            c = remote(
                self.total.at[:, theirs],
                self.total.at[:, theirs],
                self.sems.at[6, j],
                self.sems.at[7, j],
                "dp",
                self.mate,
            )
            c.start()
            forwards.append(c)
        self.gather_copies[0].wait()
        for c in forwards:
            c.wait()


def contract(former, latter, dims):
    return lax.dot_general(former, latter, (dims, ((), ())), preferred_element_type=F32)


def kernel(
    n_sec,
    n_dp,
    seq_len,
    lengths_ref,
    logits_hbm,
    hidden_ref,
    down_ref,
    up_hbm,
    ids_ref,
    values_ref,
    other_ref,
    loss_ref,
    a_total,
    b_total,
    logits_ref,
    up_ref,
    load_sems,
    scores_ref,
    teach_ref,
    grad_ref,
    hi_ref,
    lo_ref,
    piece_ref,
    low_buf,
    stat_buf,
    back_buf,
    acc_ref,
    row_ref,
    b_part,
    b_pair,
    b_slots,
    a_part,
    a_pair,
    a_slots,
    loss_part,
    loss_slots,
    sec_send,
    sec_recv,
    b_sems,
    a_sems,
    loss_sems,
):
    rows, width = logits_ref.shape
    features = hidden_ref.shape[1]
    topk = ids_ref.shape[1]
    rank = up_ref.shape[0]
    blocks = width // LANES
    sec = lax.axis_index("section")
    me = lax.axis_index("dp")
    n2 = n_dp // 2
    core = lax.rem(me, 2)
    chip = me // 2
    mate = me + 1 - 2 * core

    logits_load = pltpu.make_async_copy(logits_hbm, logits_ref, load_sems.at[0])
    up_load = pltpu.make_async_copy(up_hbm, up_ref, load_sems.at[1])
    up_load.start()
    logits_load.start()
    barrier = pltpu.get_barrier_semaphore()
    for j in range(1, n_sec):
        pl.semaphore_signal(barrier, inc=1, device_id={"section": lax.rem(sec + j, n_sec)}, device_id_type=MESH)
    pl.semaphore_signal(barrier, inc=1, device_id={"dp": mate}, device_id_type=MESH)
    for j in range(1, n2):
        pl.semaphore_signal(
            barrier, inc=1, device_id={"dp": lax.rem(chip + j, n2) * 2 + core}, device_id_type=MESH
        )

    low_part = contract(hidden_ref[...], down_ref[...], ((1,), (1,)))
    low_buf[sec] = low_part.astype(BF16)
    pl.semaphore_wait(barrier, n_sec - 1 + 1 + n2 - 1)
    low_swap = SectionExchange(low_buf, sec_send.at[0], sec_recv.at[0], n_sec)
    low_swap.start()

    seq_total = rows // seq_len
    values = jnp.concatenate([values_ref[s].T for s in range(seq_total)], axis=0)
    eye = lax.broadcasted_iota(jnp.int32, (seq_len, seq_len), 0) == lax.broadcasted_iota(
        jnp.int32, (seq_len, seq_len), 1
    )
    rest = jnp.concatenate(
        [
            jnp.sum(jnp.where(eye, jnp.broadcast_to(other_ref[s : s + 1, :], (seq_len, seq_len)), 0.0), axis=1, keepdims=True)
            for s in range(seq_total)
        ],
        axis=0,
    )
    teacher_top = jnp.maximum(jnp.max(values, axis=1, keepdims=True), rest)
    teacher_norm = (
        jnp.log(jnp.sum(jnp.exp(values - teacher_top), axis=1, keepdims=True) + jnp.exp(rest - teacher_top))
        + teacher_top
    )
    log_t_tail = rest - teacher_norm
    shifted = jnp.minimum(values - teacher_norm, 0.0) - 1.0
    first = shifted.astype(BF16).astype(F32)
    second = (shifted - first).astype(BF16).astype(F32)
    third = shifted - first - second
    ids = jnp.concatenate([ids_ref[s].T for s in range(seq_total)], axis=0)
    high = ((ids >> 7) - sec * blocks).astype(F32)
    low = (ids & (LANES - 1)).astype(F32)
    hi_ref[...] = jnp.full((rows, LANES), -1.0, F32)
    lo_ref[...] = jnp.full((rows, LANES), -1.0, F32)
    piece_ref[...] = jnp.zeros((rows, LANES), F32)
    for i, piece in enumerate((first, second, third)):
        span = slice(i * topk, (i + 1) * topk)
        hi_ref[:, span] = high
        lo_ref[:, span] = low
        piece_ref[:, span] = piece
    block_iota = lax.broadcasted_iota(jnp.int32, (blocks, LANES), 0).astype(F32)
    lane_iota = lax.broadcasted_iota(jnp.int32, (LANES, LANES), 0).astype(F32)

    def place_row(r):
        left = jnp.where(block_iota == hi_ref[pl.ds(r, 1), :], piece_ref[pl.ds(r, 1), :], 0.0)
        right = jnp.where(lane_iota == lo_ref[pl.ds(r, 1), :], 1.0, 0.0)
        teach_ref[pl.ds(r, blocks, stride=rows), :] = contract(
            left.astype(BF16), right.astype(BF16), ((1,), (1,))
        )

    unroll = UNROLL

    @pl.loop(0, rows // unroll)
    def _(step):
        for u in range(unroll):
            place_row(step * unroll + u)

    low_swap.wait()
    up_load.wait()
    logits_load.wait()
    low_sum = low_buf[0].astype(F32)
    for s in range(1, n_sec):
        low_sum = low_sum + low_buf[s].astype(F32)
    low_rank = low_sum.astype(BF16)
    low_rank_t = low_sum.T.astype(BF16)

    span = SPAN

    def score_step(step, top):
        cols = pl.ds(pl.multiple_of(step * span, span), span)
        block = logits_ref[:, cols].astype(F32) + jnp.dot(
            low_rank, up_ref[:, cols], preferred_element_type=F32
        )
        scores_ref[:, cols] = block
        for i in range(span // LANES):
            top = jnp.maximum(top, block[:, i * LANES : (i + 1) * LANES])
        return top

    top = lax.fori_loop(
        0, width // span, score_step, jnp.full((rows, LANES), -3.0e38, F32), unroll=2
    )
    local_top = jnp.max(top, axis=1, keepdims=True)
    row_ref[0] = jnp.broadcast_to(local_top, (rows, LANES))

    group = 32
    lane = lax.broadcasted_iota(jnp.int32, (group, LANES), 1)
    chunk = 4

    @pl.loop(0, rows // group)
    def _(g):
        base = pl.multiple_of(g * group, group)
        here = pl.ds(base, group)
        peak = row_ref[0, here, :]

        def step_sum(step, carry):
            total, tail, mass, cross = carry
            for i in range(chunk):
                b = step * chunk + i
                s = scores_ref[here, pl.ds(pl.multiple_of(b * LANES, LANES), LANES)]
                t = teach_ref[pl.ds(pl.multiple_of(b * rows + base, group), group), :]
                gap = s - peak
                e = jnp.exp(gap)
                named = t < 0.0
                e_named = jnp.where(named, e, 0.0)
                total = total + e
                tail = tail + jnp.where(named, 0.0, e)
                mass = mass + e_named
                cross = cross + e_named * (gap - t)
            return total, tail, mass, cross

        zero = jnp.zeros((group, LANES), F32)
        sums = lax.fori_loop(0, blocks // chunk, step_sum, (zero, zero, zero, zero))
        packed = peak
        for i, x in enumerate(sums):
            packed = jnp.where(lane == i + 1, jnp.sum(x, axis=1, keepdims=True), packed)
        stat_buf[sec, here, :] = packed

    stat_swap = SectionExchange(stat_buf, sec_send.at[1], sec_recv.at[1], n_sec)
    stat_swap.start()
    position = lax.broadcasted_iota(jnp.int32, (seq_len, 1), 0)
    valid = jnp.concatenate(
        [(position < lengths_ref[s]).astype(F32) for s in range(seq_total)], axis=0
    )
    count = lengths_ref[0]
    for s in range(1, seq_total):
        count = count + lengths_ref[s]
    stat_swap.wait()

    tops = [stat_buf[s, :, 0:1] for s in range(n_sec)]
    row_top = functools.reduce(jnp.maximum, tops)
    shrink = [jnp.exp(t - row_top) for t in tops]
    row_total = sum(stat_buf[s, :, 1:2] * shrink[s] for s in range(n_sec))
    tail_mass = sum(stat_buf[s, :, 2:3] * shrink[s] for s in range(n_sec))
    log_total = jnp.log(row_total)
    log_tail = jnp.log(tail_mass) - log_total
    tail_ratio = log_tail - log_t_tail
    divergence = jnp.exp(log_tail) * tail_ratio
    for s in range(n_sec):
        shift = tops[s] - row_top - log_total - 1.0
        divergence = divergence + (shrink[s] / row_total) * (
            stat_buf[s, :, 4:5] + stat_buf[s, :, 3:4] * shift
        )
    own_shift = local_top - row_top - log_total - 1.0
    full = (rows, LANES)
    row_ref[1] = jnp.broadcast_to(valid * jnp.exp(local_top - row_top) / row_total, full)
    row_ref[2] = jnp.broadcast_to(own_shift - divergence, full)
    row_ref[3] = jnp.broadcast_to(tail_ratio - divergence, full)

    loss_sum = jnp.sum(valid * divergence, axis=0, keepdims=True)
    tile_lane = lax.broadcasted_iota(jnp.int32, (8, LANES), 1)
    loss_part[0] = jnp.where(tile_lane == 0, loss_sum, jnp.where(tile_lane == 1, count.astype(F32), 0.0))
    loss_pair = remote(loss_part.at[0], loss_part.at[1], loss_sems.at[0, 0], loss_sems.at[1, 0], "dp", mate)
    loss_pair.start()

    acc_ref[...] = jnp.zeros_like(acc_ref)
    if b_part.shape[1] > width:
        b_part[:, width:] = jnp.zeros((rank, b_part.shape[1] - width), BF16)
    if a_part.shape[1] > features:
        a_part[:, features:] = jnp.zeros((rank, a_part.shape[1] - features), BF16)
    b_sum = DataReduce(b_part, b_pair, b_slots, b_total, b_sems, n_dp)
    a_sum = DataReduce(a_part, a_pair, a_slots, a_total, a_sems, n_dp)
    wide = grad_ref.shape[1]

    def grad_step(step):
        for g in range(rows // group):
            here = pl.ds(g * group, group)
            peak, scale = row_ref[0, here, :], row_ref[1, here, :]
            named_add, tail_add = row_ref[2, here, :], row_ref[3, here, :]
            for i in range(wide // LANES):
                b = step * (wide // LANES) + i
                s = scores_ref[here, pl.ds(pl.multiple_of(b * LANES, LANES), LANES)]
                t = teach_ref[pl.ds(pl.multiple_of(b * rows + g * group, group), group), :]
                gap = s - peak
                coef = jnp.where(t < 0.0, gap - t + named_add, tail_add)
                grad_ref[here, i * LANES : (i + 1) * LANES] = (jnp.exp(gap) * scale * coef).astype(BF16)
        cols = pl.ds(pl.multiple_of(step * wide, wide), wide)
        g_block = grad_ref[...]
        acc_ref[...] += contract(g_block, up_ref[:, cols], ((1,), (1,)))
        b_part[:, cols] = jnp.dot(low_rank_t, g_block, preferred_element_type=F32).astype(BF16)

    def grad_piece(half, piece):
        first_step = (half * b_sum.half + piece * b_sum.width) // wide

        @pl.when(first_step * wide < width)
        def _():
            for i in range(b_sum.width // wide):
                grad_step(first_step + i)

    @pl.loop(0, n2)
    def _(i):
        j = lax.rem(i + 1, n2)
        grad_piece(1 - core, lax.rem(chip + j, n2))
        b_sum.pair_copy(j).start()

    @pl.loop(0, n2)
    def _(i):
        j = lax.rem(i + 1, n2)
        grad_piece(core, lax.rem(chip + j, n2))
        b_sum.merge_piece(j)

        @pl.when(i < n2 - 1)
        def _():
            b_sum.scatter_copy(j).start()

    back_buf[sec] = acc_ref[...].astype(BF16)
    back_swap = SectionExchange(back_buf, sec_send.at[2], sec_recv.at[2], n_sec)
    back_swap.start()

    loss_pair.wait()
    loss_part[2] = loss_part[0] + loss_part[1]
    loss_copies = []
    for j in range(1, n2):
        c = remote(
            loss_part.at[2],
            loss_slots.at[j - 1],
            loss_sems.at[0, j],
            loss_sems.at[1, j],
            "dp",
            lax.rem(chip + j, n2) * 2 + core,
        )
        c.start()
        loss_copies.append(c)

    back_swap.wait()
    back_sum = back_buf[0].astype(F32)
    for s in range(1, n_sec):
        back_sum = back_sum + back_buf[s].astype(F32)
    back_t = back_sum.T.astype(BF16)
    a_part[:, 0:features] = jnp.dot(back_t, hidden_ref[...], preferred_element_type=F32).astype(BF16)
    a_sum.start_pair()
    a_sum.start_scatter()
    b_sum.start_gather()
    a_sum.start_gather()

    loss_all = loss_part[2]
    for j in range(1, n2):
        loss_copies[j - 1].wait()
        loss_all = loss_all + loss_slots[j - 1]
    loss_ref[...] = loss_all

    b_sum.forward()
    a_sum.forward()


def scale_kernel(sums_ref, a_ref, b_ref, loss_ref, grad_a_ref, grad_b_ref):
    count = sums_ref[0:1, 1:2]
    factor = SCALE_LOSS / count
    loss_ref[...] = sums_ref[0:1, 0:1] / count
    grad_a_ref[...] = a_ref[...].astype(F32) * factor
    grad_b_ref[...] = b_ref[...].astype(F32) * factor


def padded(columns, n):
    unit = LANES * n
    return (columns + unit - 1) // unit * unit


def body(
    n_sec,
    n_dp,
    student_head_logits,
    hidden,
    adapter_down,
    adapter_up,
    teacher_top_index,
    teacher_top_values,
    teacher_other_logit,
    lengths,
):
    seq_total, seq_len, width = student_head_logits.shape
    rows = seq_total * seq_len
    features = hidden.shape[2]
    topk = teacher_top_index.shape[2]
    rank = adapter_up.shape[0]
    n2 = n_dp // 2
    b_width, a_width = padded(width, n_dp), padded(features, n_dp)
    vmem = pl.BlockSpec(memory_space=pltpu.VMEM)
    hbm = pl.BlockSpec(memory_space=pltpu.HBM)

    def reduce_scratch(columns):
        return [
            pltpu.VMEM((rank, columns), BF16),
            pltpu.VMEM((rank, columns // 2), BF16),
            pltpu.VMEM((n2 - 1, rank, columns // n_dp), BF16),
        ]

    sums, a_total, b_total = pl.pallas_call(
        functools.partial(kernel, n_sec, n_dp, seq_len),
        out_shape=(
            jax.ShapeDtypeStruct((8, LANES), F32),
            jax.ShapeDtypeStruct((rank, a_width), BF16),
            jax.ShapeDtypeStruct((rank, b_width), BF16),
        ),
        in_specs=[pl.BlockSpec(memory_space=pltpu.SMEM), hbm, vmem, vmem, hbm] + [vmem] * 3,
        out_specs=(vmem, vmem, vmem),
        scratch_shapes=[
            pltpu.VMEM((rows, width), BF16),
            pltpu.VMEM((rank, width), BF16),
            pltpu.SemaphoreType.DMA((2,)),
            pltpu.VMEM((rows, width), F32),
            pltpu.VMEM((rows * (width // LANES), LANES), F32),
            pltpu.VMEM((rows, min(1024, b_width // n_dp)), BF16),
            pltpu.VMEM((rows, LANES), F32),
            pltpu.VMEM((rows, LANES), F32),
            pltpu.VMEM((rows, LANES), F32),
            pltpu.VMEM((n_sec, rows, rank), BF16),
            pltpu.VMEM((n_sec, rows, LANES), F32),
            pltpu.VMEM((n_sec, rows, rank), BF16),
            pltpu.VMEM((rows, rank), F32),
            pltpu.VMEM((4, rows, LANES), F32),
            *reduce_scratch(b_width),
            *reduce_scratch(a_width),
            pltpu.VMEM((3, 8, LANES), F32),
            pltpu.VMEM((n2 - 1, 8, LANES), F32),
            pltpu.SemaphoreType.DMA((3, n_sec - 1)),
            pltpu.SemaphoreType.DMA((3, n_sec - 1)),
            pltpu.SemaphoreType.DMA((8, n2)),
            pltpu.SemaphoreType.DMA((8, n2)),
            pltpu.SemaphoreType.DMA((2, n2)),
        ],
        compiler_params=pltpu.CompilerParams(
            collective_id=0, has_side_effects=True, vmem_limit_bytes=60 * 1024 * 1024
        ),
    )(
        lengths,
        student_head_logits.reshape(rows, width),
        hidden.reshape(rows, features),
        adapter_down.T,
        adapter_up,
        jnp.swapaxes(teacher_top_index, 1, 2),
        jnp.swapaxes(teacher_top_values, 1, 2),
        teacher_other_logit,
    )
    loss, grad_a, grad_b = pl.pallas_call(
        scale_kernel,
        out_shape=(
            jax.ShapeDtypeStruct((1, 1), F32),
            jax.ShapeDtypeStruct((rank, features), F32),
            jax.ShapeDtypeStruct((rank, width), F32),
        ),
        grid=(SCALE_STEPS,),
        in_specs=[
            pl.BlockSpec((8, LANES), lambda i: (0, 0)),
            pl.BlockSpec((rank, features // SCALE_STEPS), lambda i: (0, i)),
            pl.BlockSpec((rank, width // SCALE_STEPS), lambda i: (0, i)),
        ],
        out_specs=(
            pl.BlockSpec((1, 1), lambda i: (0, 0)),
            pl.BlockSpec((rank, features // SCALE_STEPS), lambda i: (0, i)),
            pl.BlockSpec((rank, width // SCALE_STEPS), lambda i: (0, i)),
        ),
    )(sums, a_total, b_total)
    return (loss[0, 0], grad_a.T, grad_b)


def solution(mesh):
    return jax.shard_map(
        functools.partial(body, mesh.shape["section"], mesh.shape["dp"]),
        mesh=mesh,
        in_specs=(
            P("dp", None, "section"),
            P("dp", None, "section"),
            P("section", None),
            P(None, "section"),
            P("dp", None, None),
            P("dp", None, None),
            P("dp", None),
            P("dp"),
        ),
        out_specs=(P(), P("section", None), P(None, "section")),
        check_vma=False,
    )
```

```python
import functools

import jax
import jax.numpy as jnp
from jax import lax
from jax.experimental import pallas as pl
from jax.experimental.pallas import tpu as pltpu
from jax.sharding import PartitionSpec as P

SCALE_LOSS = 16384.0
LANES = 128
SPAN = 2048
UNROLL = 32
SCALE_STEPS = 2
F32 = jnp.float32
BF16 = jnp.bfloat16
MESH = pl.DeviceIdType.MESH


def remote(src, dst, send, recv, axis, target):
    return pltpu.make_async_remote_copy(
        src_ref=src,
        dst_ref=dst,
        send_sem=send,
        recv_sem=recv,
        device_id={axis: target},
        device_id_type=MESH,
    )


class SectionExchange:
    def __init__(self, buf, send, recv, n):
        self.buf = buf
        me = lax.axis_index("section")
        self.copies = [
            remote(buf.at[me], buf.at[me], send.at[j - 1], recv.at[j - 1], "section", lax.rem(me + j, n))
            for j in range(1, n)
        ]

    def start(self):
        for c in self.copies:
            c.start()

    def wait(self):
        for c in self.copies:
            c.wait()


class DataReduce:
    def __init__(self, part, pair, slots, total, sems, n):
        self.part, self.pair, self.slots, self.total = part, pair, slots, total
        self.sems = sems
        self.n2 = n // 2
        self.width = part.shape[1] // n
        self.half = part.shape[1] // 2
        me = lax.axis_index("dp")
        self.core = lax.rem(me, 2)
        self.chip = me // 2
        self.mate = me + 1 - 2 * self.core

    def peer(self, j):
        return lax.rem(self.chip + j, self.n2) * 2 + self.core

    def cols(self, half, piece):
        start = pl.multiple_of(half * self.half + piece * self.width, LANES)
        return pl.ds(start, self.width)

    def order(self):
        return list(range(1, self.n2)) + [0]

    def pair_copy(self, j):
        piece = lax.rem(self.chip + j, self.n2)
        return remote(
            self.part.at[:, self.cols(1 - self.core, piece)],
            self.pair.at[:, self.cols(0, piece)],
            self.sems.at[0, j],
            self.sems.at[1, j],
            "dp",
            self.mate,
        )

    def start_pair(self):
        for j in self.order():
            self.pair_copy(j).start()

    def merge_piece(self, j):
        piece = lax.rem(self.chip + j, self.n2)
        self.pair_copy(j).wait()
        mine = self.cols(self.core, piece)
        both = self.part[:, mine].astype(F32) + self.pair[:, self.cols(0, piece)].astype(F32)
        self.part[:, mine] = both.astype(BF16)

    def scatter_copy(self, j):
        piece = lax.rem(self.chip + j, self.n2)
        return remote(
            self.part.at[:, self.cols(self.core, piece)],
            self.slots.at[j - 1],
            self.sems.at[2, j],
            self.sems.at[3, j],
            "dp",
            self.peer(j),
        )

    def start_scatter(self):
        for j in self.order():
            self.merge_piece(j)
            if j:
                self.scatter_copy(j).start()

    def start_gather(self):
        mine = self.cols(self.core, self.chip)
        acc = self.part[:, mine].astype(F32)
        for j in range(1, self.n2):
            self.scatter_copy(j).wait()
            acc = acc + self.slots[j - 1].astype(F32)
        self.total[:, mine] = acc.astype(BF16)
        self.gather_copies = {}
        for j in self.order():
            c = remote(
                self.total.at[:, mine],
                self.total.at[:, mine],
                self.sems.at[4, j],
                self.sems.at[5, j],
                "dp",
                self.peer(j) if j else self.mate,
            )
            c.start()
            self.gather_copies[j] = c

    def forward(self):
        forwards = []
        for j in range(1, self.n2):
            piece = lax.rem(self.chip + self.n2 - j, self.n2)
            theirs = self.cols(self.core, piece)
            self.gather_copies[j].wait()
            c = remote(
                self.total.at[:, theirs],
                self.total.at[:, theirs],
                self.sems.at[6, j],
                self.sems.at[7, j],
                "dp",
                self.mate,
            )
            c.start()
            forwards.append(c)
        self.gather_copies[0].wait()
        for c in forwards:
            c.wait()


def contract(former, latter, dims):
    return lax.dot_general(former, latter, (dims, ((), ())), preferred_element_type=F32)


def kernel(
    n_sec,
    n_dp,
    seq_len,
    lengths_ref,
    logits_hbm,
    hidden_ref,
    down_ref,
    up_hbm,
    ids_ref,
    values_ref,
    other_ref,
    loss_ref,
    a_total,
    b_total,
    logits_ref,
    up_ref,
    load_sems,
    scores_ref,
    teach_ref,
    grad_ref,
    hi_ref,
    lo_ref,
    piece_ref,
    low_buf,
    stat_buf,
    back_buf,
    acc_ref,
    row_ref,
    b_part,
    b_pair,
    b_slots,
    a_part,
    a_pair,
    a_slots,
    loss_part,
    loss_slots,
    sec_send,
    sec_recv,
    b_sems,
    a_sems,
    loss_sems,
):
    rows, width = logits_ref.shape
    features = hidden_ref.shape[1]
    topk = ids_ref.shape[1]
    rank = up_ref.shape[0]
    blocks = width // LANES
    sec = lax.axis_index("section")
    me = lax.axis_index("dp")
    n2 = n_dp // 2
    core = lax.rem(me, 2)
    chip = me // 2
    mate = me + 1 - 2 * core

    logits_load = pltpu.make_async_copy(logits_hbm, logits_ref, load_sems.at[0])
    up_load = pltpu.make_async_copy(up_hbm, up_ref, load_sems.at[1])
    up_load.start()
    logits_load.start()
    barrier = pltpu.get_barrier_semaphore()
    for j in range(1, n_sec):
        pl.semaphore_signal(barrier, inc=1, device_id={"section": lax.rem(sec + j, n_sec)}, device_id_type=MESH)
    pl.semaphore_signal(barrier, inc=1, device_id={"dp": mate}, device_id_type=MESH)
    for j in range(1, n2):
        pl.semaphore_signal(
            barrier, inc=1, device_id={"dp": lax.rem(chip + j, n2) * 2 + core}, device_id_type=MESH
        )

    low_part = contract(hidden_ref[...], down_ref[...], ((1,), (1,)))
    low_buf[sec] = low_part.astype(BF16)
    pl.semaphore_wait(barrier, n_sec - 1 + 1 + n2 - 1)
    low_swap = SectionExchange(low_buf, sec_send.at[0], sec_recv.at[0], n_sec)
    low_swap.start()

    seq_total = rows // seq_len
    values = jnp.concatenate([values_ref[s].T for s in range(seq_total)], axis=0)
    eye = lax.broadcasted_iota(jnp.int32, (seq_len, seq_len), 0) == lax.broadcasted_iota(
        jnp.int32, (seq_len, seq_len), 1
    )
    rest = jnp.concatenate(
        [
            jnp.sum(jnp.where(eye, jnp.broadcast_to(other_ref[s : s + 1, :], (seq_len, seq_len)), 0.0), axis=1, keepdims=True)
            for s in range(seq_total)
        ],
        axis=0,
    )
    teacher_top = jnp.maximum(jnp.max(values, axis=1, keepdims=True), rest)
    teacher_norm = (
        jnp.log(jnp.sum(jnp.exp(values - teacher_top), axis=1, keepdims=True) + jnp.exp(rest - teacher_top))
        + teacher_top
    )
    log_t_tail = rest - teacher_norm
    shifted = jnp.minimum(values - teacher_norm, 0.0) - 1.0
    first = shifted.astype(BF16).astype(F32)
    second = (shifted - first).astype(BF16).astype(F32)
    third = shifted - first - second
    ids = jnp.concatenate([ids_ref[s].T for s in range(seq_total)], axis=0)
    high = ((ids >> 7) - sec * blocks).astype(F32)
    low = (ids & (LANES - 1)).astype(F32)
    hi_ref[...] = jnp.full((rows, LANES), -1.0, F32)
    lo_ref[...] = jnp.full((rows, LANES), -1.0, F32)
    piece_ref[...] = jnp.zeros((rows, LANES), F32)
    for i, piece in enumerate((first, second, third)):
        span = slice(i * topk, (i + 1) * topk)
        hi_ref[:, span] = high
        lo_ref[:, span] = low
        piece_ref[:, span] = piece
    block_iota = lax.broadcasted_iota(jnp.int32, (blocks, LANES), 0).astype(F32)
    lane_iota = lax.broadcasted_iota(jnp.int32, (LANES, LANES), 0).astype(F32)

    def place_row(r):
        left = jnp.where(block_iota == hi_ref[pl.ds(r, 1), :], piece_ref[pl.ds(r, 1), :], 0.0)
        right = jnp.where(lane_iota == lo_ref[pl.ds(r, 1), :], 1.0, 0.0)
        teach_ref[pl.ds(r, blocks, stride=rows), :] = contract(
            left.astype(BF16), right.astype(BF16), ((1,), (1,))
        )

    unroll = UNROLL

    @pl.loop(0, rows // unroll)
    def _(step):
        for u in range(unroll):
            place_row(step * unroll + u)

    low_swap.wait()
    up_load.wait()
    logits_load.wait()
    low_sum = low_buf[0].astype(F32)
    for s in range(1, n_sec):
        low_sum = low_sum + low_buf[s].astype(F32)
    low_rank = low_sum.astype(BF16)
    low_rank_t = low_sum.T.astype(BF16)

    span = SPAN

    def score_step(step, top):
        cols = pl.ds(pl.multiple_of(step * span, span), span)
        block = logits_ref[:, cols].astype(F32) + jnp.dot(
            low_rank, up_ref[:, cols], preferred_element_type=F32
        )
        scores_ref[:, cols] = block
        for i in range(span // LANES):
            top = jnp.maximum(top, block[:, i * LANES : (i + 1) * LANES])
        return top

    top = lax.fori_loop(
        0, width // span, score_step, jnp.full((rows, LANES), -3.0e38, F32), unroll=2
    )
    local_top = jnp.max(top, axis=1, keepdims=True)
    row_ref[0] = jnp.broadcast_to(local_top, (rows, LANES))

    group = 32
    lane = lax.broadcasted_iota(jnp.int32, (group, LANES), 1)
    chunk = 8

    @pl.loop(0, rows // group)
    def _(g):
        base = pl.multiple_of(g * group, group)
        here = pl.ds(base, group)
        peak = row_ref[0, here, :]

        def step_sum(step, carry):
            total, tail, mass, cross = carry
            for i in range(chunk):
                b = step * chunk + i
                s = scores_ref[here, pl.ds(pl.multiple_of(b * LANES, LANES), LANES)]
                t = teach_ref[pl.ds(pl.multiple_of(b * rows + base, group), group), :]
                gap = s - peak
                e = jnp.exp(gap)
                named = t < 0.0
                e_named = jnp.where(named, e, 0.0)
                total = total + e
                tail = tail + jnp.where(named, 0.0, e)
                mass = mass + e_named
                cross = cross + e_named * (gap - t)
            return total, tail, mass, cross

        zero = jnp.zeros((group, LANES), F32)
        sums = lax.fori_loop(0, blocks // chunk, step_sum, (zero, zero, zero, zero))
        packed = peak
        for i, x in enumerate(sums):
            packed = jnp.where(lane == i + 1, jnp.sum(x, axis=1, keepdims=True), packed)
        stat_buf[sec, here, :] = packed

    stat_swap = SectionExchange(stat_buf, sec_send.at[1], sec_recv.at[1], n_sec)
    stat_swap.start()
    position = lax.broadcasted_iota(jnp.int32, (seq_len, 1), 0)
    valid = jnp.concatenate(
        [(position < lengths_ref[s]).astype(F32) for s in range(seq_total)], axis=0
    )
    count = lengths_ref[0]
    for s in range(1, seq_total):
        count = count + lengths_ref[s]
    stat_swap.wait()

    tops = [stat_buf[s, :, 0:1] for s in range(n_sec)]
    row_top = functools.reduce(jnp.maximum, tops)
    shrink = [jnp.exp(t - row_top) for t in tops]
    row_total = sum(stat_buf[s, :, 1:2] * shrink[s] for s in range(n_sec))
    tail_mass = sum(stat_buf[s, :, 2:3] * shrink[s] for s in range(n_sec))
    log_total = jnp.log(row_total)
    log_tail = jnp.log(tail_mass) - log_total
    tail_ratio = log_tail - log_t_tail
    divergence = jnp.exp(log_tail) * tail_ratio
    for s in range(n_sec):
        shift = tops[s] - row_top - log_total - 1.0
        divergence = divergence + (shrink[s] / row_total) * (
            stat_buf[s, :, 4:5] + stat_buf[s, :, 3:4] * shift
        )
    own_shift = local_top - row_top - log_total - 1.0
    full = (rows, LANES)
    row_ref[1] = jnp.broadcast_to(valid * jnp.exp(local_top - row_top) / row_total, full)
    row_ref[2] = jnp.broadcast_to(own_shift - divergence, full)
    row_ref[3] = jnp.broadcast_to(tail_ratio - divergence, full)

    loss_sum = jnp.sum(valid * divergence, axis=0, keepdims=True)
    tile_lane = lax.broadcasted_iota(jnp.int32, (8, LANES), 1)
    loss_part[0] = jnp.where(tile_lane == 0, loss_sum, jnp.where(tile_lane == 1, count.astype(F32), 0.0))
    loss_pair = remote(loss_part.at[0], loss_part.at[1], loss_sems.at[0, 0], loss_sems.at[1, 0], "dp", mate)
    loss_pair.start()

    acc_ref[...] = jnp.zeros_like(acc_ref)
    if b_part.shape[1] > width:
        b_part[:, width:] = jnp.zeros((rank, b_part.shape[1] - width), BF16)
    if a_part.shape[1] > features:
        a_part[:, features:] = jnp.zeros((rank, a_part.shape[1] - features), BF16)
    b_sum = DataReduce(b_part, b_pair, b_slots, b_total, b_sems, n_dp)
    a_sum = DataReduce(a_part, a_pair, a_slots, a_total, a_sems, n_dp)
    wide = grad_ref.shape[1]

    def grad_step(step):
        for g in range(rows // group):
            here = pl.ds(g * group, group)
            peak, scale = row_ref[0, here, :], row_ref[1, here, :]
            named_add, tail_add = row_ref[2, here, :], row_ref[3, here, :]
            for i in range(wide // LANES):
                b = step * (wide // LANES) + i
                s = scores_ref[here, pl.ds(pl.multiple_of(b * LANES, LANES), LANES)]
                t = teach_ref[pl.ds(pl.multiple_of(b * rows + g * group, group), group), :]
                gap = s - peak
                coef = jnp.where(t < 0.0, gap - t + named_add, tail_add)
                grad_ref[here, i * LANES : (i + 1) * LANES] = (jnp.exp(gap) * scale * coef).astype(BF16)
        cols = pl.ds(pl.multiple_of(step * wide, wide), wide)
        g_block = grad_ref[...]
        acc_ref[...] += contract(g_block, up_ref[:, cols], ((1,), (1,)))
        b_part[:, cols] = jnp.dot(low_rank_t, g_block, preferred_element_type=F32).astype(BF16)

    def grad_piece(half, piece):
        first_step = (half * b_sum.half + piece * b_sum.width) // wide

        @pl.when(first_step * wide < width)
        def _():
            for i in range(b_sum.width // wide):
                grad_step(first_step + i)

    @pl.loop(0, n2)
    def _(i):
        j = lax.rem(i + 1, n2)
        grad_piece(1 - core, lax.rem(chip + j, n2))
        b_sum.pair_copy(j).start()

    @pl.loop(0, n2)
    def _(i):
        j = lax.rem(i + 1, n2)
        grad_piece(core, lax.rem(chip + j, n2))
        b_sum.merge_piece(j)

        @pl.when(i < n2 - 1)
        def _():
            b_sum.scatter_copy(j).start()

    back_buf[sec] = acc_ref[...].astype(BF16)
    back_swap = SectionExchange(back_buf, sec_send.at[2], sec_recv.at[2], n_sec)
    back_swap.start()

    loss_pair.wait()
    loss_part[2] = loss_part[0] + loss_part[1]
    loss_copies = []
    for j in range(1, n2):
        c = remote(
            loss_part.at[2],
            loss_slots.at[j - 1],
            loss_sems.at[0, j],
            loss_sems.at[1, j],
            "dp",
            lax.rem(chip + j, n2) * 2 + core,
        )
        c.start()
        loss_copies.append(c)

    back_swap.wait()
    back_sum = back_buf[0].astype(F32)
    for s in range(1, n_sec):
        back_sum = back_sum + back_buf[s].astype(F32)
    back_t = back_sum.T.astype(BF16)
    a_part[:, 0:features] = jnp.dot(back_t, hidden_ref[...], preferred_element_type=F32).astype(BF16)
    a_sum.start_pair()
    a_sum.start_scatter()
    b_sum.start_gather()
    a_sum.start_gather()

    loss_all = loss_part[2]
    for j in range(1, n2):
        loss_copies[j - 1].wait()
        loss_all = loss_all + loss_slots[j - 1]
    loss_ref[...] = loss_all

    b_sum.forward()
    a_sum.forward()


def scale_kernel(sums_ref, a_ref, b_ref, loss_ref, grad_a_ref, grad_b_ref):
    count = sums_ref[0:1, 1:2]
    factor = SCALE_LOSS / count
    loss_ref[...] = sums_ref[0:1, 0:1] / count
    grad_a_ref[...] = a_ref[...].astype(F32) * factor
    grad_b_ref[...] = b_ref[...].astype(F32) * factor


def padded(columns, n):
    unit = LANES * n
    return (columns + unit - 1) // unit * unit


def body(
    n_sec,
    n_dp,
    student_head_logits,
    hidden,
    adapter_down,
    adapter_up,
    teacher_top_index,
    teacher_top_values,
    teacher_other_logit,
    lengths,
):
    seq_total, seq_len, width = student_head_logits.shape
    rows = seq_total * seq_len
    features = hidden.shape[2]
    topk = teacher_top_index.shape[2]
    rank = adapter_up.shape[0]
    n2 = n_dp // 2
    b_width, a_width = padded(width, n_dp), padded(features, n_dp)
    vmem = pl.BlockSpec(memory_space=pltpu.VMEM)
    hbm = pl.BlockSpec(memory_space=pltpu.HBM)

    def reduce_scratch(columns):
        return [
            pltpu.VMEM((rank, columns), BF16),
            pltpu.VMEM((rank, columns // 2), BF16),
            pltpu.VMEM((n2 - 1, rank, columns // n_dp), BF16),
        ]

    sums, a_total, b_total = pl.pallas_call(
        functools.partial(kernel, n_sec, n_dp, seq_len),
        out_shape=(
            jax.ShapeDtypeStruct((8, LANES), F32),
            jax.ShapeDtypeStruct((rank, a_width), BF16),
            jax.ShapeDtypeStruct((rank, b_width), BF16),
        ),
        in_specs=[pl.BlockSpec(memory_space=pltpu.SMEM), hbm, vmem, vmem, hbm] + [vmem] * 3,
        out_specs=(vmem, vmem, vmem),
        scratch_shapes=[
            pltpu.VMEM((rows, width), BF16),
            pltpu.VMEM((rank, width), BF16),
            pltpu.SemaphoreType.DMA((2,)),
            pltpu.VMEM((rows, width), F32),
            pltpu.VMEM((rows * (width // LANES), LANES), F32),
            pltpu.VMEM((rows, min(1024, b_width // n_dp)), BF16),
            pltpu.VMEM((rows, LANES), F32),
            pltpu.VMEM((rows, LANES), F32),
            pltpu.VMEM((rows, LANES), F32),
            pltpu.VMEM((n_sec, rows, rank), BF16),
            pltpu.VMEM((n_sec, rows, LANES), F32),
            pltpu.VMEM((n_sec, rows, rank), BF16),
            pltpu.VMEM((rows, rank), F32),
            pltpu.VMEM((4, rows, LANES), F32),
            *reduce_scratch(b_width),
            *reduce_scratch(a_width),
            pltpu.VMEM((3, 8, LANES), F32),
            pltpu.VMEM((n2 - 1, 8, LANES), F32),
            pltpu.SemaphoreType.DMA((3, n_sec - 1)),
            pltpu.SemaphoreType.DMA((3, n_sec - 1)),
            pltpu.SemaphoreType.DMA((8, n2)),
            pltpu.SemaphoreType.DMA((8, n2)),
            pltpu.SemaphoreType.DMA((2, n2)),
        ],
        compiler_params=pltpu.CompilerParams(
            collective_id=0, has_side_effects=True, vmem_limit_bytes=60 * 1024 * 1024
        ),
    )(
        lengths,
        student_head_logits.reshape(rows, width),
        hidden.reshape(rows, features),
        adapter_down.T,
        adapter_up,
        jnp.swapaxes(teacher_top_index, 1, 2),
        jnp.swapaxes(teacher_top_values, 1, 2),
        teacher_other_logit,
    )
    loss, grad_a, grad_b = pl.pallas_call(
        scale_kernel,
        out_shape=(
            jax.ShapeDtypeStruct((1, 1), F32),
            jax.ShapeDtypeStruct((rank, features), F32),
            jax.ShapeDtypeStruct((rank, width), F32),
        ),
        grid=(SCALE_STEPS,),
        in_specs=[
            pl.BlockSpec((8, LANES), lambda i: (0, 0)),
            pl.BlockSpec((rank, features // SCALE_STEPS), lambda i: (0, i)),
            pl.BlockSpec((rank, width // SCALE_STEPS), lambda i: (0, i)),
        ],
        out_specs=(
            pl.BlockSpec((1, 1), lambda i: (0, 0)),
            pl.BlockSpec((rank, features // SCALE_STEPS), lambda i: (0, i)),
            pl.BlockSpec((rank, width // SCALE_STEPS), lambda i: (0, i)),
        ),
    )(sums, a_total, b_total)
    return (loss[0, 0], grad_a.T, grad_b)


def solution(mesh):
    return jax.shard_map(
        functools.partial(body, mesh.shape["section"], mesh.shape["dp"]),
        mesh=mesh,
        in_specs=(
            P("dp", None, "section"),
            P("dp", None, "section"),
            P("section", None),
            P(None, "section"),
            P("dp", None, None),
            P("dp", None, None),
            P("dp", None),
            P("dp"),
        ),
        out_specs=(P(), P("section", None), P(None, "section")),
        check_vma=False,
    )
```
